32 devices in a mesh: row: 8 (over z, x), col: 4 (over y, core).
Axes of the slice: x: 2, y: 2, z: 4, core: 2. Of those that a mesh axis runs over, the one named last changes fastest.
Arguments:
- eigvecs: float32 [2048, 512], P('row', 'col'), may hold values from -6 to 6
- reflectors: float32 [8, 32, 128, 64], P(None, ('row', 'col')), may hold values from -2 to 2, as said below
- factors: float32 [8, 32, 64, 64], P(None, ('row', 'col')), may hold values from -3 to 3, as said below
- order: int32 [8], replicated, may hold values from 0 to 7, each once
- offsets: int32 [8], replicated, may hold values from 0 to 63
Outputs:
- rotated: float32 [2048, 512], P('row', 'col')
The draws below stay inside these ranges and needn't reach their ends.
Inputs may be any that keep to these rules, and one draw needn't show every extreme that they name: `order`: a permutation of 0 .. 7. Every block map is orthogonal: with V the block of reflectors and T the block of factors, T is upper triangular and T^-1 + T^-T = V^T V. `factors`: upper triangular, paired with reflectors as promised there.
All inputs are finite; a program needn't handle non-finite values.
Results may differ from the reference program's by a relative error of at most 0.0003.
Values sent between devices are 32-bit elements; how exact they have to be, the bound alone decides.
A program may use at most 64 MiB of HBM per device.

```python
import jax
import jax.numpy as jnp
from jax import lax

NB = 64
SWEEPS = 8
NBLK = 32
ORDER = 2048
VECS = 512


def build_pair(key):
    inner_key = jax.random.fold_in(key, 11)
    spread = 0.03
    identity = jnp.eye(NB, dtype=jnp.float32)
    base = jnp.concatenate([identity, -identity], 0)
    noise = jax.random.normal(inner_key, (SWEEPS, NBLK, 2 * NB, NB), jnp.float32) * spread
    householder = base + noise
    gram = jnp.einsum('abik,abil->abkl', householder, householder, precision=lax.Precision.HIGHEST)
    inverse_factor = jnp.triu(gram, 1) + gram * identity * 0.5
    triangle = lax.linalg.triangular_solve(inverse_factor, jnp.broadcast_to(identity, inverse_factor.shape), left_side=True, lower=False)
    return (householder, triangle)


def draw_reflectors(key, part):
    return build_pair(key)[0]


def draw_factors(key, part):
    return build_pair(key)[1]


def with_ends(drawn, own_key, smallest, top_value):
    longest = drawn.shape.index(max(drawn.shape))
    spots = []
    for shift in (0, 1):
        where = [jax.random.randint(jax.random.fold_in(own_key, axis), (), 0, length) for axis, length in enumerate(drawn.shape)]
        where[longest] = (where[longest] + shift) % drawn.shape[longest]
        spots.append(tuple(where))
    return drawn.at[spots[0]].set(smallest).at[spots[1]].set(top_value)


def block_scale(stream_key, extent, cuts, least, largest):
    def one(dim, shards_of):
        heights = jax.random.uniform(jax.random.fold_in(jax.random.fold_in(stream_key, 6), dim), (shards_of,), jnp.float32, least / len(cuts), largest / len(cuts))
        return jnp.repeat(jnp.exp(heights), extent[dim] // shards_of).reshape((-1,) + (1,) * (len(extent) - dim - 1))

    loudness = one(*cuts[0])
    for cut in cuts[1:]:
        loudness = loudness * one(*cut)
    return loudness


def centred(stream_key, extent, scale, limit, split=(), kind=jnp.bfloat16):
    factor_of = block_scale(stream_key, extent, split, -0.22, 0.18) if split else 1.0
    entries = jax.random.normal(stream_key, extent, jnp.float32) * scale * factor_of
    return jnp.minimum(jnp.maximum(entries, -limit), limit).astype(kind)


def setup_inputs(seed: int = 0) -> dict:
    key_list = jax.random.split(jax.random.key(seed), 6)
    return {
        "eigvecs": centred(key_list[0], (ORDER, VECS), 1.0, 6.0, ((0, 8), (1, 4)), jnp.float32),
        "reflectors": draw_reflectors(jax.random.fold_in(key_list[5], 71), 0),
        "factors": draw_factors(jax.random.fold_in(key_list[5], 71), 0),
        "order": jax.random.permutation(key_list[3], SWEEPS).astype(jnp.int32),
        "offsets": with_ends(jax.random.randint(key_list[4], (SWEEPS,), 0, NB), jax.random.fold_in(key_list[4], 1), 0, NB - 1).astype(jnp.int32),
    }


highest = lax.Precision.HIGHEST

def reflect(segment, householder, triangle):
    inner = jnp.dot(householder.T.astype(jnp.float32), segment.astype(jnp.float32), precision=highest, preferred_element_type=jnp.float32)
    inner = jnp.dot(triangle.astype(jnp.float32), inner.astype(jnp.float32), precision=highest, preferred_element_type=jnp.float32)
    return segment - jnp.dot(householder.astype(jnp.float32), inner.astype(jnp.float32), precision=highest, preferred_element_type=jnp.float32)

def reference(eigvecs, reflectors, factors, order, offsets):
    height = eigvecs.shape[0]
    columns = eigvecs.shape[1]
    number_blocks = reflectors.shape[1]
    vectors = eigvecs
    for position in range(SWEEPS):
        stored = order[position].astype(jnp.int32)
        offset = offsets[stored].astype(jnp.int32)
        house_set = lax.dynamic_index_in_dim(reflectors, stored, 0, keepdims=False)
        tri_set = lax.dynamic_index_in_dim(factors, stored, 0, keepdims=False)
        padded = jnp.concatenate([vectors, jnp.zeros((2 * NB, columns), jnp.float32)], 0)

        def advance(number, current):
            start = (offset + number * NB).astype(jnp.int32)
            segment = lax.dynamic_slice_in_dim(current, start, 2 * NB, 0)
            householder = lax.dynamic_index_in_dim(house_set, number, 0, keepdims=False)
            triangle = lax.dynamic_index_in_dim(tri_set, number, 0, keepdims=False)
            return lax.dynamic_update_slice_in_dim(current, reflect(segment, householder, triangle), start, 0)
        padded = lax.fori_loop(0, number_blocks, advance, padded)
        vectors = padded[:height]
    return vectors
```

```python
import functools

import jax
import jax.numpy as jnp
from jax import lax
from jax.experimental import pallas as pl
from jax.experimental.pallas import tpu as pltpu
from jax.sharding import PartitionSpec as P

highest = lax.Precision.HIGHEST
LAG = 3


def split(x):
    hi = x.astype(jnp.bfloat16)
    lo = (x - hi.astype(jnp.float32)).astype(jnp.bfloat16)
    return hi, lo


def product(a, b):
    a_hi, a_lo = split(a)
    b_hi, b_lo = split(b)
    dot = functools.partial(jnp.dot, preferred_element_type=jnp.float32)
    return dot(a_hi, b_hi) + (dot(a_hi, b_lo) + dot(a_lo, b_hi))


def wave(sweeps, blocks, width, order_ref, off_ref, x_ref, *refs):
    maps, (out_ref, frames, carry) = refs[:sweeps], refs[sweeps:]
    step = pl.program_id(0)
    height = x_ref.shape[0]
    pad = 2 * width

    @pl.when(step == 0)
    def _():
        frames[0, pl.ds(pad, height), :] = x_ref[...]

    loaded = []
    for p in range(sweeps):
        k = step - 2 - LAG * p
        here = off_ref[order_ref[p]]
        before = off_ref[order_ref[p - 1]] if p else 0
        at = jnp.clip(k, -2, blocks - 1)
        rows = frames[p, pl.ds((at + 1) * width + here - before + pad, width), :]
        index = (at + 1) * width + here + lax.broadcasted_iota(jnp.int32, rows.shape, 0)
        rows = jnp.where(index < height, rows, 0.0)
        loaded.append(jnp.concatenate([carry[p], rows], 0))
    results = []
    for p in range(sweeps):
        k = step - 2 - LAG * p
        moved = product(maps[p][0, 0], loaded[p])
        results.append(jnp.where(k >= 0, moved, loaded[p]))
    for p in range(sweeps):
        k = step - 2 - LAG * p
        spot = jnp.clip(k, -2, blocks) + 2
        frames[p + 1, pl.ds(pl.multiple_of(spot * width, width), width), :] = results[p][:width]
        carry[p] = results[p][width:]

    @pl.when(step == pl.num_programs(0) - 1)
    def _():
        last = off_ref[order_ref[sweeps - 1]]

        def put(n, _):
            at = pl.multiple_of(n * width, width)
            out_ref[pl.ds(at, width), :] = frames[sweeps, pl.ds(at + pad - last, width), :]
            return 0

        lax.fori_loop(0, height // width, put, 0)


def sweep_all(vectors, maps, order, offsets):
    blocks, sweeps, span, _ = maps.shape
    width = span // 2
    height, columns = vectors.shape
    steps = blocks + 2 + LAG * (sweeps - 1)

    def map_spec(p):
        return pl.BlockSpec(
            (1, 1, span, span),
            lambda w, *_: (jnp.clip(w - 2 - LAG * p, 0, blocks - 1), p, 0, 0),
        )

    return pl.pallas_call(
        functools.partial(wave, sweeps, blocks, width),
        out_shape=jax.ShapeDtypeStruct((height, columns), jnp.float32),
        grid_spec=pltpu.PrefetchScalarGridSpec(
            num_scalar_prefetch=2,
            grid=(steps,),
            in_specs=[pl.BlockSpec((height, columns), lambda w, *_: (0, 0))]
            + [map_spec(p) for p in range(sweeps)],
            out_specs=pl.BlockSpec((height, columns), lambda w, *_: (0, 0)),
            scratch_shapes=[
                pltpu.VMEM((sweeps + 1, (blocks + 5) * width, columns), jnp.float32),
                pltpu.VMEM((sweeps, width, columns), jnp.float32),
            ],
        ),
        compiler_params=pltpu.CompilerParams(dimension_semantics=("arbitrary",)),
    )(order, offsets, vectors, *([maps] * sweeps))


def wavefront(eigvecs, reflectors, factors, order, offsets):
    house = reflectors[order, 0]
    tri = factors[order, 0]
    scaled = jnp.einsum("sab,sbc->sac", house, tri, precision=highest)
    inner = jnp.einsum("sab,scb->sac", scaled, house, precision=highest)
    own = jnp.eye(inner.shape[-1], dtype=jnp.float32) - inner
    maps = lax.all_gather(own, ("row", "col"), axis=0, tiled=False)
    strip = lax.all_to_all(eigvecs, "row", split_axis=1, concat_axis=0, tiled=True)
    moved = sweep_all(strip, maps, order, offsets)
    return lax.all_to_all(moved, "row", split_axis=0, concat_axis=1, tiled=True)


def passed_along(block, axis, distance):
    devices = range(lax.axis_size(axis))
    route = [(i - distance, i) for i in devices if i - distance in devices]
    return lax.ppermute(block, axis, route)


def entering(array, axis, combine, identity):
    size, position = (lax.axis_size(axis), lax.axis_index(axis))
    everything = jax.tree.map(lambda part: lax.all_gather(part, axis), array)
    start = jax.tree.map(
        lambda part, zero: jnp.broadcast_to(jnp.asarray(zero, part.dtype), part.shape),
        array,
        identity,
    )

    def hop(k, before):
        reached = k < position
        new = combine(before, jax.tree.map(lambda part: part[k], everything))
        return jax.tree.map(lambda a, b: jnp.where(reached, a, b), new, before)

    return lax.fori_loop(0, size, hop, start)


def reflect(segment, householder, triangle):
    inner = jnp.dot(householder.T, segment, precision=highest, preferred_element_type=jnp.float32)
    inner = jnp.dot(triangle, inner, precision=highest, preferred_element_type=jnp.float32)
    return segment - jnp.dot(
        householder, inner, precision=highest, preferred_element_type=jnp.float32
    )


def sweep_apply(extended, house_set, tri_set, offset):
    block_width = house_set.shape[-1]

    def advance(number, current):
        start = offset + number * block_width
        segment = lax.dynamic_slice_in_dim(current, start, 2 * block_width, 0)
        householder = lax.dynamic_index_in_dim(house_set, number, 0, keepdims=False)
        triangle = lax.dynamic_index_in_dim(tri_set, number, 0, keepdims=False)
        return lax.dynamic_update_slice_in_dim(
            current, reflect(segment, householder, triangle), start, 0
        )

    return lax.fori_loop(0, house_set.shape[0], advance, extended)


def compose(earlier, later):
    first_map = jnp.dot(later[0], earlier[0], precision=highest, preferred_element_type=jnp.float32)
    shifted = (
        jnp.dot(later[0], earlier[1], precision=highest, preferred_element_type=jnp.float32)
        + later[1]
    )
    return (first_map, shifted)


def local(eigvecs, reflectors, factors, order, offsets):
    height = eigvecs.shape[0]
    columns = eigvecs.shape[1]
    block_width = reflectors.shape[-1]
    span_rows = 2 * block_width
    leading = lax.axis_index("row") == 0
    identity = jnp.eye(span_rows, dtype=jnp.float32)
    probe = jnp.concatenate([identity, jnp.zeros((height, span_rows), jnp.float32)], 0)
    vectors = eigvecs
    for position in range(order.shape[0]):
        stored = order[position]
        offset = offsets[stored]
        own_house = lax.dynamic_index_in_dim(reflectors, stored, 0, keepdims=False)
        own_tri = lax.dynamic_index_in_dim(factors, stored, 0, keepdims=False)
        house_set, tri_set = (
            lax.all_gather(own_house, "col", axis=0, tiled=True),
            lax.all_gather(own_tri, "col", axis=0, tiled=True),
        )
        next_rows = passed_along(vectors[:span_rows], "row", -1)
        top_rows = jnp.where(leading, vectors[:span_rows], 0.0)
        extended = jnp.concatenate([top_rows, vectors[span_rows:], next_rows], 0)
        joined = sweep_apply(jnp.concatenate([extended, probe], 1), house_set, tri_set, offset)
        partial_value = joined[:, :columns]
        response = joined[:, columns:]
        transfer = jnp.where(leading, 0.0, response[height:])
        empty = jnp.zeros((span_rows, columns), jnp.float32)
        composed = entering((transfer, partial_value[height:]), "row", compose, (identity, empty))
        incoming = composed[1]
        vectors = partial_value[:height] + jnp.dot(
            response[:height], incoming, precision=highest, preferred_element_type=jnp.float32
        )
    return vectors


def solution(mesh):
    placed = (
        P("row", "col"),
        P(None, ("row", "col"), None, None),
        P(None, ("row", "col"), None, None),
        P(),
        P(),
    )

    def run(eigvecs, reflectors, factors, order, offsets):
        sweeps, count, span, _ = reflectors.shape
        gathered = 4 * sweeps * count * mesh.size * span * span
        fits = gathered <= 24 * 2**20 and eigvecs.shape[1] % mesh.shape["row"] == 0 and count == 1
        body = wavefront if fits else local
        return body(eigvecs, reflectors, factors, order, offsets)

    return jax.shard_map(
        run, mesh=mesh, in_specs=placed, out_specs=P("row", "col"), check_vma=False
    )
```

```python
import functools

import jax
import jax.numpy as jnp
from jax import lax
from jax.experimental import pallas as pl
from jax.experimental.pallas import tpu as pltpu
from jax.sharding import PartitionSpec as P

MESH = pl.DeviceIdType.MESH
highest = lax.Precision.HIGHEST


def split(x):
    hi = x.astype(jnp.bfloat16)
    lo = (x - hi.astype(jnp.float32)).astype(jnp.bfloat16)
    return hi, lo


def product(a, b):
    a_hi, a_lo = split(a)
    b_hi, b_lo = split(b)
    dot = functools.partial(jnp.dot, preferred_element_type=jnp.float32)
    return dot(a_hi, b_hi) + (dot(a_hi, b_lo) + dot(a_lo, b_hi))


def kernel(
    rows_n, cols_n, order_ref, off_ref, x_ref, house_ref, tri_ref, out_ref,
    maps, frames, up_in, down_in, down_out, last_in,
    map_send, map_recv, up_send, up_recv, down_send, down_recv, last_send, last_recv,
):
    row, col = lax.axis_index("row"), lax.axis_index("col")
    sweeps, span = maps.shape[1], maps.shape[2]
    width = span // 2
    height, columns = x_ref.shape
    per = height // width
    pad = span
    first, final = row == 0, row == rows_n - 1

    def peer(shift):
        return lax.rem(col + shift, cols_n)

    def map_copy(p, shift):
        return pltpu.make_async_remote_copy(
            src_ref=maps.at[col, p], dst_ref=maps.at[col, p],
            send_sem=map_send.at[shift - 1, p], recv_sem=map_recv.at[col, p],
            device_id=(row, peer(shift)), device_id_type=MESH,
        )

    def map_arrival(p, j):
        return pltpu.make_async_remote_copy(
            src_ref=maps.at[j, p], dst_ref=maps.at[j, p],
            send_sem=map_send.at[0, p], recv_sem=map_recv.at[j, p],
            device_id=(row, j), device_id_type=MESH,
        )

    def up_copy(q, part, src):
        return pltpu.make_async_remote_copy(
            src_ref=src, dst_ref=up_in.at[q, part],
            send_sem=up_send.at[q, part], recv_sem=up_recv.at[q, part],
            device_id=(row - 1, col), device_id_type=MESH,
        )

    def down_copy(q):
        return pltpu.make_async_remote_copy(
            src_ref=down_out.at[q], dst_ref=down_in.at[q],
            send_sem=down_send.at[q], recv_sem=down_recv.at[q],
            device_id=(row + 1, col), device_id_type=MESH,
        )

    def last_copy():
        return pltpu.make_async_remote_copy(
            src_ref=frames.at[sweeps, pl.ds(pad + height - width, width)], dst_ref=last_in,
            send_sem=last_send, recv_sem=last_recv,
            device_id=(row + 1, col), device_id_type=MESH,
        )

    def frame(q, part):
        return frames.at[q, pl.ds(pad + part * width, width)]

    barrier = pltpu.get_barrier_semaphore()
    for shift in range(1, cols_n):
        pl.semaphore_signal(barrier, inc=1, device_id=(row, peer(shift)), device_id_type=MESH)

    @pl.when(row > 0)
    def _():
        pl.semaphore_signal(barrier, inc=1, device_id=(row - 1, col), device_id_type=MESH)

    @pl.when(row < rows_n - 1)
    def _():
        pl.semaphore_signal(barrier, inc=1, device_id=(row + 1, col), device_id_type=MESH)

    def dense(p):
        house = house_ref[order_ref[p], 0]
        tri = tri_ref[order_ref[p], 0]
        scaled = jnp.dot(house, tri, precision=highest, preferred_element_type=jnp.float32)
        inner = lax.dot_general(
            scaled, house, (((1,), (1,)), ((), ())), precision=highest,
            preferred_element_type=jnp.float32,
        )
        eye = lax.broadcasted_iota(jnp.int32, inner.shape, 0) == lax.broadcasted_iota(
            jnp.int32, inner.shape, 1
        )
        maps[col, p] = jnp.where(eye, 1.0, 0.0) - inner

    dense(0)
    frames[0, pl.ds(pad, height), :] = x_ref[...]
    greeted = cols_n - 1 + jnp.minimum(row, 1) + jnp.minimum(rows_n - 1 - row, 1)
    pl.semaphore_wait(barrier, greeted)

    for shift in range(1, cols_n):
        map_copy(0, shift).start()

    @pl.when(row > 0)
    def _():
        for part in range(2):
            up_copy(0, part, x_ref.at[pl.ds(part * width, width)]).start()

    def spread(p, _):
        dense(p)
        for shift in range(1, cols_n):
            map_copy(p, shift).start()
        return 0

    lax.fori_loop(1, sweeps, spread, 0)

    def sweep(q, _):
        here = off_ref[order_ref[q]]
        before = jnp.where(q == 0, 0, off_ref[order_ref[jnp.maximum(q - 1, 0)]])
        move = here - before
        for j in range(cols_n):

            @pl.when(col != j)
            def _(j=j):
                map_arrival(q, j).wait_recv()

        def fresh(j):
            rows = frames[q, pl.ds(pad + (j + 1) * width + move, width), :]
            index = row * height + (j + 1) * width + here
            index = index + lax.broadcasted_iota(jnp.int32, rows.shape, 0)
            return jnp.where(index < rows_n * height, rows, 0.0)

        blank = jnp.zeros((width, columns), jnp.float32)

        def early(j):
            return product(maps[j, q], jnp.concatenate([blank, fresh(j)], 0))

        def late(j, ready, carried):
            return ready + product(maps[j, q], jnp.concatenate([carried, blank], 0))

        def arrive(part):
            @pl.when(row < rows_n - 1)
            def _():
                up_copy(q, part, up_in.at[q, part]).wait_recv()

            frames[q, pl.ds(pad + height + part * width, width), :] = up_in[q, part]

        ready = [early(j) for j in range(per - 2)]
        top = frames[q, pl.ds(pad - width + move, width), :]
        frames[q + 1, pl.ds(pad - width, width), :] = top
        own = frames[q, pl.ds(pad + move, width), :]

        @pl.when(row > 0)
        def _():
            down_copy(q).wait_recv()

        carried = jnp.where(first, own, down_in[q])
        for j in range(per):
            if j >= per - 2:
                arrive(j - (per - 2))
                ready.append(early(j))
            both = late(j, ready[j], carried)
            frames[q + 1, pl.ds(pad + j * width, width), :] = both[:width]
            carried = both[width:]
            if j < 2:

                @pl.when((row > 0) & (q < sweeps - 1))
                def _(j=j):
                    up_copy(q + 1, j, frame(q + 1, j)).start()

        down_out[q] = carried

        @pl.when(row < rows_n - 1)
        def _():
            down_copy(q).start()

        return 0

    lax.fori_loop(0, sweeps, sweep, 0)

    @pl.when(row < rows_n - 1)
    def _():
        last_copy().start()

    @pl.when(row > 0)
    def _():
        last_copy().wait_recv()

    edge = frames[sweeps, pl.ds(pad - width, width), :]
    frames[sweeps, pl.ds(pad - width, width), :] = jnp.where(first, edge, last_in[...])
    shift_back = off_ref[order_ref[sweeps - 1]]
    out_ref[...] = frames[sweeps, pl.ds(pad - shift_back, height), :]

    def drain(p, _):
        for shift in range(1, cols_n):
            map_copy(p, shift).wait_send()

        @pl.when(row > 0)
        def _():
            for part in range(2):
                up_copy(p, part, up_in.at[p, part]).wait_send()

        @pl.when(row < rows_n - 1)
        def _():
            down_copy(p).wait_send()

        return 0

    lax.fori_loop(0, sweeps, drain, 0)

    @pl.when(row < rows_n - 1)
    def _():
        last_copy().wait_send()


def local(rows_n, cols_n, eigvecs, reflectors, factors, order, offsets):
    sweeps, _, span, width = reflectors.shape
    height, columns = eigvecs.shape
    part = (width, columns)
    vmem = pl.BlockSpec(memory_space=pltpu.VMEM)
    smem = pl.BlockSpec(memory_space=pltpu.SMEM)
    dma = pltpu.SemaphoreType.DMA
    return pl.pallas_call(
        functools.partial(kernel, rows_n, cols_n),
        out_shape=jax.ShapeDtypeStruct((height, columns), jnp.float32),
        in_specs=[smem, smem, vmem, vmem, vmem],
        out_specs=vmem,
        scratch_shapes=[
            pltpu.VMEM((cols_n, sweeps, span, span), jnp.float32),
            pltpu.VMEM((sweeps + 1, height + 2 * span, columns), jnp.float32),
            pltpu.VMEM((sweeps, 2) + part, jnp.float32),
            pltpu.VMEM((sweeps,) + part, jnp.float32),
            pltpu.VMEM((sweeps,) + part, jnp.float32),
            pltpu.VMEM(part, jnp.float32),
            dma((cols_n - 1, sweeps)),
            dma((cols_n, sweeps)),
            dma((sweeps, 2)),
            dma((sweeps, 2)),
            dma((sweeps,)),
            dma((sweeps,)),
            dma,
            dma,
        ],
        compiler_params=pltpu.CompilerParams(collective_id=0, has_side_effects=True),
    )(order, offsets, eigvecs, reflectors, factors)


def solution(mesh):
    placed = (
        P("row", "col"),
        P(None, ("row", "col"), None, None),
        P(None, ("row", "col"), None, None),
        P(),
        P(),
    )
    body = functools.partial(local, mesh.shape["row"], mesh.shape["col"])
    return jax.shard_map(
        body, mesh=mesh, in_specs=placed, out_specs=P("row", "col"), check_vma=False
    )
```

```python
import functools

import jax
import jax.numpy as jnp
from jax import lax
from jax.experimental import pallas as pl
from jax.experimental.pallas import tpu as pltpu
from jax.sharding import PartitionSpec as P

MESH = pl.DeviceIdType.MESH
highest = lax.Precision.HIGHEST


def split(x):
    hi = x.astype(jnp.bfloat16)
    lo = (x - hi.astype(jnp.float32)).astype(jnp.bfloat16)
    return hi, lo


def product(a, b):
    a_hi, a_lo = split(a)
    b_hi, b_lo = split(b)
    dot = functools.partial(jnp.dot, preferred_element_type=jnp.float32)
    return dot(a_hi, b_hi) + (dot(a_hi, b_lo) + dot(a_lo, b_hi))


def kernel(
    rows_n, cols_n, order_ref, off_ref, x_ref, house_ref, tri_ref, out_ref,
    maps, frames, up_in, down_in, down_out, last_in,
    map_send, map_recv, extra_send, extra_recv,
    up_send, up_recv, down_send, down_recv, last_send, last_recv,
):
    row, col = lax.axis_index("row"), lax.axis_index("col")
    sweeps, span = maps.shape[1], maps.shape[2]
    pairs = sweeps // 2
    width = span // 2
    height, columns = x_ref.shape
    per = height // width
    pad = span
    first = row == 0
    above, below = row > 0, row < rows_n - 1
    odd = lax.rem(col, 2)
    near = col + 1 - 2 * odd
    far = lax.rem(col + cols_n // 2, cols_n)
    low = col < 2

    def send(src, dst, sent, got, to_row, to_col):
        return pltpu.make_async_remote_copy(
            src_ref=src, dst_ref=dst, send_sem=sent, recv_sem=got,
            device_id=(to_row, to_col), device_id_type=MESH,
        )

    def map_copy(kind, p):
        slot = far if kind == 2 else col
        place = maps.at[slot, p]
        to = far if kind == 1 else near
        return send(place, place, map_send.at[kind, p], map_recv.at[slot, p], row, to)

    def map_arrival(j, p):
        return send(maps.at[j, p], maps.at[j, p], map_send.at[0, p], map_recv.at[j, p], row, near)

    def extra_up(t):
        return send(
            maps.at[col, 2 * t], maps.at[cols_n + odd, 2 * t],
            extra_send.at[0, t], extra_recv.at[odd, t], row - 1, col,
        )

    def extra_copy(kind, t, slot):
        place = maps.at[cols_n + slot, 2 * t]
        to = far if kind == 2 else near
        return send(place, place, extra_send.at[kind, t], extra_recv.at[slot, t], row, to)

    def up_copy(t, part, src):
        return send(
            src, up_in.at[t, part], up_send.at[t, part], up_recv.at[t, part], row - 1, col
        )

    def down_copy(q):
        return send(
            down_out.at[q], down_in.at[q], down_send.at[q], down_recv.at[q], row + 1, col
        )

    def last_copy():
        return send(
            frames.at[sweeps, pl.ds(pad + height - width, width)], last_in,
            last_send, last_recv, row + 1, col,
        )

    barrier = pltpu.get_barrier_semaphore()

    def greet(to_row, to_col):
        pl.semaphore_signal(
            barrier, inc=1, device_id=(to_row, to_col), device_id_type=MESH
        )

    greet(row, near)
    greet(row, far)

    @pl.when(above)
    def _():
        greet(row - 1, col)

    @pl.when(below)
    def _():
        greet(row + 1, col)

    def dense(p):
        house = house_ref[order_ref[p], 0]
        tri = tri_ref[order_ref[p], 0]
        scaled = jnp.dot(house, tri, precision=highest, preferred_element_type=jnp.float32)
        inner = lax.dot_general(
            scaled, house, (((1,), (1,)), ((), ())), precision=highest,
            preferred_element_type=jnp.float32,
        )
        eye = lax.broadcasted_iota(jnp.int32, inner.shape, 0) == lax.broadcasted_iota(
            jnp.int32, inner.shape, 1
        )
        maps[col, p] = jnp.where(eye, 1.0, 0.0) - inner

    dense(0)
    frames[0, pl.ds(pad, height), :] = x_ref[...]
    greeted = 2 + jnp.minimum(row, 1) + jnp.minimum(rows_n - 1 - row, 1)
    pl.semaphore_wait(barrier, greeted)
    map_copy(1, 0).start()
    map_copy(0, 0).start()

    @pl.when(above)
    def _():
        for part in range(per):
            up_copy(0, part, x_ref.at[pl.ds(part * width, width)]).start()

    @pl.when(above & low)
    def _():
        extra_up(0).start()

    def spread(p, _):
        dense(p)
        map_copy(1, p).start()
        map_copy(0, p).start()

        @pl.when(above & low & (lax.rem(p, 2) == 0))
        def _():
            extra_up(p // 2).start()

        return 0

    def relay(t):
        for q in (2 * t, 2 * t + 1):
            map_arrival(far, q).wait_recv()
            map_copy(2, q).start()

        @pl.when(below)
        def _():
            extra_copy(1, t, odd).wait_recv()
            extra_copy(1, t, odd).start()

            @pl.when(low)
            def _():
                extra_copy(2, t, odd).start()

    lax.fori_loop(1, sweeps, spread, 0)
    relay(0)

    blank = jnp.zeros((width, columns), jnp.float32)

    def pair(t, _):
        a, b = 2 * t, 2 * t + 1
        start_a, start_b = off_ref[order_ref[a]], off_ref[order_ref[b]]
        before = jnp.where(t == 0, 0, off_ref[order_ref[jnp.maximum(a - 1, 0)]])
        shift = {0: start_a - before, 1: start_b - start_a}
        start = {0: start_a, 1: start_b}
        for q in (a, b):
            for j in range(cols_n):

                @pl.when((col != j) & (far != j))
                def _(j=j, q=q):
                    map_arrival(j, q).wait_recv()

        @pl.when(below)
        def _():
            extra_copy(1, t, 1 - odd).wait_recv()

        def fresh(n, j):
            rows = frames[a + n, pl.ds(pad + (j + 1) * width + shift[n], width), :]
            index = row * height + (j + 1) * width + start[n]
            index = index + lax.broadcasted_iota(jnp.int32, rows.shape, 0)
            return jnp.where(index < rows_n * height, rows, 0.0)

        def early(n, j):
            return product(maps[j, a + n], jnp.concatenate([blank, fresh(n, j)], 0))

        def late(n, j, ready, carried):
            return ready + product(maps[j, a + n], jnp.concatenate([carried, blank], 0))

        def put(n, j, value):
            frames[a + n + 1, pl.ds(pad + j * width, width), :] = value

        def arrive(part):
            @pl.when(below)
            def _():
                up_copy(t, part, up_in.at[t, part]).wait_recv()

            frames[a, pl.ds(pad + height + part * width, width), :] = up_in[t, part]

        def lead(n):
            put(n, -1, frames[a + n, pl.ds(pad - width + shift[n], width), :])
            return frames[a + n, pl.ds(pad + shift[n], width), :]

        def entry(n, own):
            @pl.when(above)
            def _():
                down_copy(a + n).wait_recv()

            return jnp.where(first, own, down_in[a + n])

        def leave(n, carried):
            down_out[a + n] = carried

            @pl.when(below)
            def _():
                down_copy(a + n).start()

        def lift(part):
            @pl.when(above & (t < pairs - 1))
            def _():
                place = frames.at[a + 2, pl.ds(pad + part * width, width)]
                up_copy(t + 1, part, place).start()

        ready = [early(0, j) for j in range(per - 2)]
        carried = entry(0, lead(0))
        for j in range(per):
            if j >= per - 2:
                arrive(j - (per - 2))
                ready.append(early(0, j))
            both = late(0, j, ready[j], carried)
            put(0, j, both[:width])
            carried = both[width:]
        leave(0, carried)

        @pl.when(t < pairs - 1)
        def _():
            relay(t + 1)

        ready = [early(1, j) for j in range(per - 2)]
        own = lead(1)
        arrive(2)
        next_ready = early(0, per)
        other = entry(1, own)
        low_out = late(1, 0, ready[0], other)
        high_out = late(0, per, next_ready, carried)
        put(0, per, high_out[:width])
        put(1, 0, low_out[:width])
        lift(0)
        arrive(3)
        next_ready = early(0, per + 1)
        high_out = late(0, per + 1, next_ready, high_out[width:])
        put(0, per + 1, high_out[:width])
        other = low_out[width:]
        for j in range(1, per):
            if j >= per - 2:
                ready.append(early(1, j))
            both = late(1, j, ready[j], other)
            put(1, j, both[:width])
            other = both[width:]
            if j < per - 1:
                lift(j)
        leave(1, other)
        lift(per - 1)
        return 0

    lax.fori_loop(0, pairs, pair, 0)

    @pl.when(below)
    def _():
        last_copy().start()

    @pl.when(above)
    def _():
        last_copy().wait_recv()

    edge = frames[sweeps, pl.ds(pad - width, width), :]
    frames[sweeps, pl.ds(pad - width, width), :] = jnp.where(first, edge, last_in[...])
    shift_back = off_ref[order_ref[sweeps - 1]]
    out_ref[...] = frames[sweeps, pl.ds(pad - shift_back, height), :]

    def drain(t, _):
        for q in (2 * t, 2 * t + 1):
            for kind in range(3):
                map_copy(kind, q).wait_send()

            @pl.when(below)
            def _(q=q):
                down_copy(q).wait_send()

        @pl.when(above)
        def _():
            for part in range(per):
                up_copy(t, part, up_in.at[t, part]).wait_send()

            @pl.when(low)
            def _():
                extra_up(t).wait_send()

        @pl.when(below)
        def _():
            extra_copy(1, t, odd).wait_send()

            @pl.when(low)
            def _():
                extra_copy(2, t, odd).wait_send()

        return 0

    lax.fori_loop(0, pairs, drain, 0)

    @pl.when(below)
    def _():
        last_copy().wait_send()


def local(rows_n, cols_n, eigvecs, reflectors, factors, order, offsets):
    sweeps, _, span, width = reflectors.shape
    height, columns = eigvecs.shape
    part = (width, columns)
    vmem = pl.BlockSpec(memory_space=pltpu.VMEM)
    smem = pl.BlockSpec(memory_space=pltpu.SMEM)
    dma = pltpu.SemaphoreType.DMA
    return pl.pallas_call(
        functools.partial(kernel, rows_n, cols_n),
        out_shape=jax.ShapeDtypeStruct((height, columns), jnp.float32),
        in_specs=[smem, smem, vmem, vmem, vmem],
        out_specs=vmem,
        scratch_shapes=[
            pltpu.VMEM((cols_n + 2, sweeps, span, span), jnp.float32),
            pltpu.VMEM((sweeps + 1, 2 * height + span, columns), jnp.float32),
            pltpu.VMEM((sweeps // 2, height // width) + part, jnp.float32),
            pltpu.VMEM((sweeps,) + part, jnp.float32),
            pltpu.VMEM((sweeps,) + part, jnp.float32),
            pltpu.VMEM(part, jnp.float32),
            dma((3, sweeps)),
            dma((cols_n, sweeps)),
            dma((3, sweeps // 2)),
            dma((2, sweeps // 2)),
            dma((sweeps // 2, height // width)),
            dma((sweeps // 2, height // width)),
            dma((sweeps,)),
            dma((sweeps,)),
            dma,
            dma,
        ],
        compiler_params=pltpu.CompilerParams(collective_id=0, has_side_effects=True),
    )(order, offsets, eigvecs, reflectors, factors)


def solution(mesh):
    placed = (
        P("row", "col"),
        P(None, ("row", "col"), None, None),
        P(None, ("row", "col"), None, None),
        P(),
        P(),
    )
    body = functools.partial(local, mesh.shape["row"], mesh.shape["col"])
    return jax.shard_map(
        body, mesh=mesh, in_specs=placed, out_specs=P("row", "col"), check_vma=False
    )
```

```python
import functools

import jax
import jax.numpy as jnp
from jax import lax
from jax.experimental import pallas as pl
from jax.experimental.pallas import tpu as pltpu
from jax.sharding import PartitionSpec as P

MESH = pl.DeviceIdType.MESH
highest = lax.Precision.HIGHEST


def split(x):
    hi = x.astype(jnp.bfloat16)
    lo = (x - hi.astype(jnp.float32)).astype(jnp.bfloat16)
    return hi, lo


def product(a, b):
    a_hi, a_lo = split(a)
    b_hi, b_lo = split(b)
    dot = functools.partial(jnp.dot, preferred_element_type=jnp.float32)
    return dot(a_hi, b_hi) + (dot(a_hi, b_lo) + dot(a_lo, b_hi))


def kernel(
    rows_n, cols_n, order_ref, off_ref, x_ref, house_ref, tri_ref, out_ref,
    maps, frames, up_in, down_in, down_out, last_in, response,
    map_send, map_recv, extra_send, extra_recv,
    up_send, up_recv, down_send, down_recv, last_send, last_recv,
):
    row, col = lax.axis_index("row"), lax.axis_index("col")
    sweeps, span = maps.shape[1], maps.shape[2]
    pairs = sweeps // 2
    width = span // 2
    height, columns = x_ref.shape
    per = height // width
    pad = span
    first = row == 0
    above, below = row > 0, row < rows_n - 1
    odd = lax.rem(col, 2)
    near = col + 1 - 2 * odd
    far = lax.rem(col + cols_n // 2, cols_n)
    low = col < 2

    def send(src, dst, sent, got, to_row, to_col):
        return pltpu.make_async_remote_copy(
            src_ref=src, dst_ref=dst, send_sem=sent, recv_sem=got,
            device_id=(to_row, to_col), device_id_type=MESH,
        )

    def map_copy(kind, p):
        slot = far if kind == 2 else col
        place = maps.at[slot, p]
        to = far if kind == 1 else near
        return send(place, place, map_send.at[kind, p], map_recv.at[slot, p], row, to)

    def map_arrival(j, p):
        return send(maps.at[j, p], maps.at[j, p], map_send.at[0, p], map_recv.at[j, p], row, near)

    def extra_up(t):
        return send(
            maps.at[col, 2 * t], maps.at[cols_n + odd, 2 * t],
            extra_send.at[0, t], extra_recv.at[odd, t], row - 1, col,
        )

    def extra_copy(kind, t, slot):
        place = maps.at[cols_n + slot, 2 * t]
        to = far if kind == 2 else near
        return send(place, place, extra_send.at[kind, t], extra_recv.at[slot, t], row, to)

    def up_copy(t, part, src):
        return send(
            src, up_in.at[t, part], up_send.at[t, part], up_recv.at[t, part], row - 1, col
        )

    def down_copy(q):
        return send(
            down_out.at[q], down_in.at[q], down_send.at[q], down_recv.at[q], row + 1, col
        )

    def last_copy():
        return send(
            frames.at[sweeps, pl.ds(pad + height - width, width)], last_in,
            last_send, last_recv, row + 1, col,
        )

    barrier = pltpu.get_barrier_semaphore()

    def greet(to_row, to_col):
        pl.semaphore_signal(
            barrier, inc=1, device_id=(to_row, to_col), device_id_type=MESH
        )

    greet(row, near)
    greet(row, far)

    @pl.when(above)
    def _():
        greet(row - 1, col)

    @pl.when(below)
    def _():
        greet(row + 1, col)

    def dense(p):
        house = house_ref[order_ref[p], 0]
        tri = tri_ref[order_ref[p], 0]
        scaled = jnp.dot(tri, house, precision=highest, preferred_element_type=jnp.float32)
        inner = lax.dot_general(
            house, scaled, (((0,), (0,)), ((), ())), precision=highest,
            preferred_element_type=jnp.float32,
        )
        eye = lax.broadcasted_iota(jnp.int32, inner.shape, 0) == lax.broadcasted_iota(
            jnp.int32, inner.shape, 1
        )
        maps[col, p] = jnp.where(eye, 1.0, 0.0) - inner

    dense(0)
    frames[0, pl.ds(pad, height), :] = x_ref[...]
    greeted = 2 + jnp.minimum(row, 1) + jnp.minimum(rows_n - 1 - row, 1)
    pl.semaphore_wait(barrier, greeted)
    map_copy(1, 0).start()
    map_copy(0, 0).start()

    @pl.when(above)
    def _():
        for part in range(per):
            up_copy(0, part, x_ref.at[pl.ds(part * width, width)]).start()

    @pl.when(above & low)
    def _():
        extra_up(0).start()

    def spread(p, _):
        dense(p)
        map_copy(1, p).start()
        map_copy(0, p).start()

        @pl.when(above & low & (lax.rem(p, 2) == 0))
        def _():
            extra_up(p // 2).start()

        return 0

    def relay(t):
        for q in (2 * t, 2 * t + 1):
            map_arrival(far, q).wait_recv()
            map_copy(2, q).start()

        @pl.when(below)
        def _():
            extra_copy(1, t, odd).wait_recv()
            extra_copy(1, t, odd).start()

            @pl.when(low)
            def _():
                extra_copy(2, t, odd).start()

    lax.fori_loop(1, sweeps, spread, 0)
    relay(0)

    blank = jnp.zeros((width, columns), jnp.float32)

    def pair(t, _):
        a, b = 2 * t, 2 * t + 1
        start_a, start_b = off_ref[order_ref[a]], off_ref[order_ref[b]]
        before = jnp.where(t == 0, 0, off_ref[order_ref[jnp.maximum(a - 1, 0)]])
        shift = {0: start_a - before, 1: start_b - start_a}
        start = {0: start_a, 1: start_b}
        for q in (a, b):
            for j in range(cols_n):

                @pl.when((col != j) & (far != j))
                def _(j=j, q=q):
                    map_arrival(j, q).wait_recv()

        @pl.when(below)
        def _():
            extra_copy(1, t, 1 - odd).wait_recv()

        def fresh(n, j):
            rows = frames[a + n, pl.ds(pad + (j + 1) * width + shift[n], width), :]
            index = row * height + (j + 1) * width + start[n]
            index = index + lax.broadcasted_iota(jnp.int32, rows.shape, 0)
            return jnp.where(index < rows_n * height, rows, 0.0)

        def early(n, j):
            return product(maps[j, a + n], jnp.concatenate([blank, fresh(n, j)], 0))

        def late(n, j, ready, carried):
            return ready + product(maps[j, a + n], jnp.concatenate([carried, blank], 0))

        def put(n, j, value):
            frames[a + n + 1, pl.ds(pad + j * width, width), :] = value

        def arrive(part):
            @pl.when(below)
            def _():
                up_copy(t, part, up_in.at[t, part]).wait_recv()

            frames[a, pl.ds(pad + height + part * width, width), :] = up_in[t, part]

        def lead(n):
            put(n, -1, frames[a + n, pl.ds(pad - width + shift[n], width), :])
            return frames[a + n, pl.ds(pad + shift[n], width), :]

        def entry(n, own):
            @pl.when(above)
            def _():
                down_copy(a + n).wait_recv()

            return jnp.where(first, own, down_in[a + n])

        def leave(n, carried):
            down_out[a + n] = carried

            @pl.when(below)
            def _():
                down_copy(a + n).start()

        def lift(part):
            @pl.when(above & (t < pairs - 1))
            def _():
                place = frames.at[a + 2, pl.ds(pad + part * width, width)]
                up_copy(t + 1, part, place).start()

        def respond(n):
            block = maps[0, a + n][:, :width]
            for j in range(per):
                if j:
                    block = product(maps[j, a + n][:, :width], block[width:])
                response[n, pl.ds(j * width, width), :] = block[:width]
            response[n, pl.ds(per * width, width), :] = block[width:]

        def idle(n, j, carried):
            ready = early(n, j)
            if carried is not None:
                ready = late(n, j, ready, carried)
            return ready

        def settle(n, parts, own):
            whole = jnp.concatenate(parts, 0) + product(response[n], entry(n, own))
            for j in range(per):
                put(n, j, whole[j * width : (j + 1) * width])
            carried = whole[per * width :]
            leave(n, carried)
            return carried

        respond(0)
        respond(1)
        parts, carried = [], None
        own = lead(0)
        for j in range(per):
            if j >= per - 2:
                arrive(j - (per - 2))
            both = idle(0, j, carried)
            parts.append(both[:width])
            carried = both[width:]
        carried = settle(0, parts + [carried], own)

        @pl.when(t < pairs - 1)
        def _():
            relay(t + 1)

        own = lead(1)
        arrive(2)
        arrive(3)
        parts, other = [], None
        for j in range(per):
            if j < 2:
                both = late(0, per + j, early(0, per + j), carried)
                put(0, per + j, both[:width])
                carried = both[width:]
            both = idle(1, j, other)
            parts.append(both[:width])
            other = both[width:]
        settle(1, parts + [other], own)
        for j in range(per):
            lift(j)
        return 0

    lax.fori_loop(0, pairs, pair, 0)

    @pl.when(below)
    def _():
        last_copy().start()

    @pl.when(above)
    def _():
        last_copy().wait_recv()

    edge = frames[sweeps, pl.ds(pad - width, width), :]
    frames[sweeps, pl.ds(pad - width, width), :] = jnp.where(first, edge, last_in[...])
    shift_back = off_ref[order_ref[sweeps - 1]]
    out_ref[...] = frames[sweeps, pl.ds(pad - shift_back, height), :]

    def drain(t, _):
        for q in (2 * t, 2 * t + 1):
            for kind in range(3):
                map_copy(kind, q).wait_send()

            @pl.when(below)
            def _(q=q):
                down_copy(q).wait_send()

        @pl.when(above)
        def _():
            for part in range(per):
                up_copy(t, part, up_in.at[t, part]).wait_send()

            @pl.when(low)
            def _():
                extra_up(t).wait_send()

        @pl.when(below)
        def _():
            extra_copy(1, t, odd).wait_send()

            @pl.when(low)
            def _():
                extra_copy(2, t, odd).wait_send()

        return 0

    lax.fori_loop(0, pairs, drain, 0)

    @pl.when(below)
    def _():
        last_copy().wait_send()


def local(rows_n, cols_n, eigvecs, reflectors, factors, order, offsets):
    sweeps, _, span, width = reflectors.shape
    height, columns = eigvecs.shape
    part = (width, columns)
    vmem = pl.BlockSpec(memory_space=pltpu.VMEM)
    smem = pl.BlockSpec(memory_space=pltpu.SMEM)
    dma = pltpu.SemaphoreType.DMA
    return pl.pallas_call(
        functools.partial(kernel, rows_n, cols_n),
        out_shape=jax.ShapeDtypeStruct((height, columns), jnp.float32),
        in_specs=[smem, smem, vmem, vmem, vmem],
        out_specs=vmem,
        scratch_shapes=[
            pltpu.VMEM((cols_n + 2, sweeps, span, span), jnp.float32),
            pltpu.VMEM((sweeps + 1, 2 * height + span, columns), jnp.float32),
            pltpu.VMEM((sweeps // 2, height // width) + part, jnp.float32),
            pltpu.VMEM((sweeps,) + part, jnp.float32),
            pltpu.VMEM((sweeps,) + part, jnp.float32),
            pltpu.VMEM(part, jnp.float32),
            pltpu.VMEM((2, height + width, width), jnp.float32),
            dma((3, sweeps)),
            dma((cols_n, sweeps)),
            dma((3, sweeps // 2)),
            dma((2, sweeps // 2)),
            dma((sweeps // 2, height // width)),
            dma((sweeps // 2, height // width)),
            dma((sweeps,)),
            dma((sweeps,)),
            dma,
            dma,
        ],
        compiler_params=pltpu.CompilerParams(collective_id=0, has_side_effects=True),
    )(order, offsets, eigvecs, jnp.swapaxes(reflectors, 2, 3), factors)


def solution(mesh):
    placed = (
        P("row", "col"),
        P(None, ("row", "col"), None, None),
        P(None, ("row", "col"), None, None),
        P(),
        P(),
    )
    body = functools.partial(local, mesh.shape["row"], mesh.shape["col"])
    return jax.shard_map(
        body, mesh=mesh, in_specs=placed, out_specs=P("row", "col"), check_vma=False
    )
```

```python
import functools

import jax
import jax.numpy as jnp
from jax import lax
from jax.experimental import pallas as pl
from jax.experimental.pallas import tpu as pltpu
from jax.sharding import PartitionSpec as P

MESH = pl.DeviceIdType.MESH
highest = lax.Precision.HIGHEST


def split(x):
    hi = x.astype(jnp.bfloat16)
    lo = (x - hi.astype(jnp.float32)).astype(jnp.bfloat16)
    return hi, lo


def product(a, b):
    a_hi, a_lo = split(a)
    b_hi, b_lo = split(b)
    dot = functools.partial(jnp.dot, preferred_element_type=jnp.float32)
    return dot(a_hi, b_hi) + (dot(a_hi, b_lo) + dot(a_lo, b_hi))


def kernel(
    rows_n, cols_n, order_ref, off_ref, x_ref, house_ref, tri_ref, out_ref,
    maps, frames, up_in, down_in, down_out, last_in, response,
    map_send, map_recv, extra_send, extra_recv,
    up_send, up_recv, down_send, down_recv, last_send, last_recv,
):
    row, col = lax.axis_index("row"), lax.axis_index("col")
    sweeps, span = maps.shape[1], maps.shape[2]
    pairs = sweeps // 2
    width = span // 2
    height, columns = x_ref.shape
    per = height // width
    pad = span
    first = row == 0
    above, below = row > 0, row < rows_n - 1
    odd = lax.rem(col, 2)
    near = col + 1 - 2 * odd
    far = lax.rem(col + cols_n // 2, cols_n)
    low = col < 2

    def send(src, dst, sent, got, to_row, to_col):
        return pltpu.make_async_remote_copy(
            src_ref=src, dst_ref=dst, send_sem=sent, recv_sem=got,
            device_id=(to_row, to_col), device_id_type=MESH,
        )

    def map_copy(kind, p):
        slot = far if kind == 2 else col
        place = maps.at[slot, p]
        to = far if kind == 1 else near
        return send(place, place, map_send.at[kind, p], map_recv.at[slot, p], row, to)

    def map_arrival(j, p):
        return send(maps.at[j, p], maps.at[j, p], map_send.at[0, p], map_recv.at[j, p], row, near)

    def extra_up(t):
        return send(
            maps.at[col, 2 * t], maps.at[cols_n + odd, 2 * t],
            extra_send.at[0, t], extra_recv.at[odd, t], row - 1, col,
        )

    def extra_copy(kind, t, slot):
        place = maps.at[cols_n + slot, 2 * t]
        to = far if kind == 2 else near
        return send(place, place, extra_send.at[kind, t], extra_recv.at[slot, t], row, to)

    def up_copy(t, part, src):
        return send(
            src, up_in.at[t, part], up_send.at[t, part], up_recv.at[t, part], row - 1, col
        )

    def down_copy(q):
        return send(
            down_out.at[q], down_in.at[q], down_send.at[q], down_recv.at[q], row + 1, col
        )

    def last_copy():
        return send(
            frames.at[sweeps, pl.ds(pad + height - width, width)], last_in,
            last_send, last_recv, row + 1, col,
        )

    barrier = pltpu.get_barrier_semaphore()

    def greet(to_row, to_col):
        pl.semaphore_signal(
            barrier, inc=1, device_id=(to_row, to_col), device_id_type=MESH
        )

    greet(row, near)
    greet(row, far)

    @pl.when(above)
    def _():
        greet(row - 1, col)

    @pl.when(below)
    def _():
        greet(row + 1, col)

    def dense(p):
        house = house_ref[order_ref[p], 0]
        tri = tri_ref[order_ref[p], 0]
        scaled = jnp.dot(tri, house, precision=highest, preferred_element_type=jnp.float32)
        inner = lax.dot_general(
            house, scaled, (((0,), (0,)), ((), ())), precision=highest,
            preferred_element_type=jnp.float32,
        )
        eye = lax.broadcasted_iota(jnp.int32, inner.shape, 0) == lax.broadcasted_iota(
            jnp.int32, inner.shape, 1
        )
        maps[col, p] = jnp.where(eye, 1.0, 0.0) - inner

    dense(0)
    frames[0, pl.ds(pad, height), :] = x_ref[...]
    greeted = 2 + jnp.minimum(row, 1) + jnp.minimum(rows_n - 1 - row, 1)
    pl.semaphore_wait(barrier, greeted)
    map_copy(1, 0).start()
    map_copy(0, 0).start()

    @pl.when(above)
    def _():
        for part in range(per):
            up_copy(0, part, x_ref.at[pl.ds(part * width, width)]).start()

    @pl.when(above & low)
    def _():
        extra_up(0).start()

    def relay(t):
        for q in (2 * t, 2 * t + 1):
            map_arrival(far, q).wait_recv()
            map_copy(2, q).start()

        @pl.when(below)
        def _():
            extra_copy(1, t, odd).wait_recv()
            extra_copy(1, t, odd).start()

            @pl.when(low)
            def _():
                extra_copy(2, t, odd).start()

    for p in range(1, sweeps):
        dense(p)
    for p in range(1, sweeps):
        map_copy(1, p).start()
        map_copy(0, p).start()

    @pl.when(above & low)
    def _():
        for t in range(1, pairs):
            extra_up(t).start()

    relay(0)

    blank = jnp.zeros((width, columns), jnp.float32)

    def pair(t, _):
        a, b = 2 * t, 2 * t + 1
        start_a, start_b = off_ref[order_ref[a]], off_ref[order_ref[b]]
        before = jnp.where(t == 0, 0, off_ref[order_ref[jnp.maximum(a - 1, 0)]])
        shift = {0: start_a - before, 1: start_b - start_a}
        start = {0: start_a, 1: start_b}
        for q in (a, b):
            for j in range(cols_n):

                @pl.when((col != j) & (far != j))
                def _(j=j, q=q):
                    map_arrival(j, q).wait_recv()

        @pl.when(below)
        def _():
            extra_copy(1, t, 1 - odd).wait_recv()

        def fresh(n, j):
            rows = frames[a + n, pl.ds(pad + (j + 1) * width + shift[n], width), :]
            index = row * height + (j + 1) * width + start[n]
            index = index + lax.broadcasted_iota(jnp.int32, rows.shape, 0)
            return jnp.where(index < rows_n * height, rows, 0.0)

        def early(n, j):
            return product(maps[j, a + n], jnp.concatenate([blank, fresh(n, j)], 0))

        def late(n, j, ready, carried):
            return ready + product(maps[j, a + n], jnp.concatenate([carried, blank], 0))

        def put(n, j, value):
            frames[a + n + 1, pl.ds(pad + j * width, width), :] = value

        def arrive(part):
            @pl.when(below)
            def _():
                up_copy(t, part, up_in.at[t, part]).wait_recv()

            frames[a, pl.ds(pad + height + part * width, width), :] = up_in[t, part]

        def lead(n):
            put(n, -1, frames[a + n, pl.ds(pad - width + shift[n], width), :])
            return frames[a + n, pl.ds(pad + shift[n], width), :]

        def entry(n, own):
            @pl.when(above)
            def _():
                down_copy(a + n).wait_recv()

            return jnp.where(first, own, down_in[a + n])

        def leave(n, carried):
            down_out[a + n] = carried

            @pl.when(below)
            def _():
                down_copy(a + n).start()

        def lift(part):
            @pl.when(above & (t < pairs - 1))
            def _():
                place = frames.at[a + 2, pl.ds(pad + part * width, width)]
                up_copy(t + 1, part, place).start()

        def respond(n):
            block = maps[0, a + n][:, :width]
            for j in range(per):
                if j:
                    block = product(maps[j, a + n][:, :width], block[width:])
                response[n, pl.ds(j * width, width), :] = block[:width]
            response[n, pl.ds(per * width, width), :] = block[width:]

        def idle(n, j, carried):
            ready = early(n, j)
            if carried is not None:
                ready = late(n, j, ready, carried)
            return ready

        def settle(n, parts, own):
            whole = jnp.concatenate(parts, 0) + product(response[n], entry(n, own))
            for j in range(per):
                put(n, j, whole[j * width : (j + 1) * width])
            carried = whole[per * width :]
            leave(n, carried)
            return carried

        respond(0)
        respond(1)
        parts, carried = [], None
        own = lead(0)
        for j in range(per):
            if j >= per - 2:
                arrive(j - (per - 2))
            both = idle(0, j, carried)
            parts.append(both[:width])
            carried = both[width:]
        carried = settle(0, parts + [carried], own)

        @pl.when(t < pairs - 1)
        def _():
            relay(t + 1)

        own = lead(1)
        arrive(2)
        arrive(3)
        parts, other = [], None
        for j in range(per):
            if j < 2:
                both = late(0, per + j, early(0, per + j), carried)
                put(0, per + j, both[:width])
                carried = both[width:]
            both = idle(1, j, other)
            parts.append(both[:width])
            other = both[width:]
        settle(1, parts + [other], own)
        for j in range(per):
            lift(j)
        return 0

    lax.fori_loop(0, pairs, pair, 0)

    @pl.when(below)
    def _():
        last_copy().start()

    @pl.when(above)
    def _():
        last_copy().wait_recv()

    edge = frames[sweeps, pl.ds(pad - width, width), :]
    frames[sweeps, pl.ds(pad - width, width), :] = jnp.where(first, edge, last_in[...])
    shift_back = off_ref[order_ref[sweeps - 1]]
    out_ref[...] = frames[sweeps, pl.ds(pad - shift_back, height), :]

    def drain(t, _):
        for q in (2 * t, 2 * t + 1):
            for kind in range(3):
                map_copy(kind, q).wait_send()

            @pl.when(below)
            def _(q=q):
                down_copy(q).wait_send()

        @pl.when(above)
        def _():
            for part in range(per):
                up_copy(t, part, up_in.at[t, part]).wait_send()

            @pl.when(low)
            def _():
                extra_up(t).wait_send()

        @pl.when(below)
        def _():
            extra_copy(1, t, odd).wait_send()

            @pl.when(low)
            def _():
                extra_copy(2, t, odd).wait_send()

        return 0

    lax.fori_loop(0, pairs, drain, 0)

    @pl.when(below)
    def _():
        last_copy().wait_send()


def local(rows_n, cols_n, eigvecs, reflectors, factors, order, offsets):
    sweeps, _, span, width = reflectors.shape
    height, columns = eigvecs.shape
    part = (width, columns)
    vmem = pl.BlockSpec(memory_space=pltpu.VMEM)
    smem = pl.BlockSpec(memory_space=pltpu.SMEM)
    dma = pltpu.SemaphoreType.DMA
    return pl.pallas_call(
        functools.partial(kernel, rows_n, cols_n),
        out_shape=jax.ShapeDtypeStruct((height, columns), jnp.float32),
        in_specs=[smem, smem, vmem, vmem, vmem],
        out_specs=vmem,
        scratch_shapes=[
            pltpu.VMEM((cols_n + 2, sweeps, span, span), jnp.float32),
            pltpu.VMEM((sweeps + 1, 2 * height + span, columns), jnp.float32),
            pltpu.VMEM((sweeps // 2, height // width) + part, jnp.float32),
            pltpu.VMEM((sweeps,) + part, jnp.float32),
            pltpu.VMEM((sweeps,) + part, jnp.float32),
            pltpu.VMEM(part, jnp.float32),
            pltpu.VMEM((2, height + width, width), jnp.float32),
            dma((3, sweeps)),
            dma((cols_n, sweeps)),
            dma((3, sweeps // 2)),
            dma((2, sweeps // 2)),
            dma((sweeps // 2, height // width)),
            dma((sweeps // 2, height // width)),
            dma((sweeps,)),
            dma((sweeps,)),
            dma,
            dma,
        ],
        compiler_params=pltpu.CompilerParams(collective_id=0, has_side_effects=True),
    )(order, offsets, eigvecs, jnp.swapaxes(reflectors, 2, 3), factors)


def solution(mesh):
    placed = (
        P("row", "col"),
        P(None, ("row", "col"), None, None),
        P(None, ("row", "col"), None, None),
        P(),
        P(),
    )
    body = functools.partial(local, mesh.shape["row"], mesh.shape["col"])
    return jax.shard_map(
        body, mesh=mesh, in_specs=placed, out_specs=P("row", "col"), check_vma=False
    )
```
